256 devices in a mesh: dp: 64 (over z, y, core), mp: 4 (over x).
Axes of the slice: x: 4, y: 4, z: 8, core: 2. Of those that a mesh axis runs over, the one named last changes fastest.
Arguments:
- latents: bfloat16 [2097152, 256], P(('dp', 'mp')), may hold values from -6 to 6
- proj_weight: bfloat16 [18, 256], replicated, may hold values from -0.375 to 0.375
- proj_bias: float32 [18], replicated, may hold values from -2.5 to 2.5
- fill: int32 [16384], replicated, may hold values from 0 to 128, as said below
- target: int32 [16384], replicated, may hold values from -1 to 63, as said below
- target_slot: int32 [16384], replicated, may hold values from -1 to 31, as said below
Outputs:
- latent_grad: bfloat16 [1048576, 256], P(('dp', 'mp'))
- weight_grad: float32 [18, 256], replicated
- entropy_loss: float32 [], replicated
The draws below stay inside these ranges and needn't reach their ends.
Inputs may be any that keep to these rules, and one draw needn't show every extreme that they name: `fill`: zero exactly on the empty slots of a device, which are those whose target is -1. `target`: blocks go to devices with the same mp index. Each device receives exactly 32 blocks, one in each of its positions; at most 1 block goes from one device to any one index of dp, and some device does send 1 block to an index. -1 marks an empty slot. `target_slot`: -1 exactly where target is -1.
All inputs are finite; a program needn't handle non-finite values.
Results may differ from the reference program's by a relative error of at most 0.0049.
Values may be sent and summed in bfloat16 or wider, within the bound.
No kernel may reach another device: no remote copies, remote signals or barrier semaphores. Data moves between devices by JAX's collectives and lax.ppermute only.
A program may use at most 64 MiB of HBM per device.

```python
import jax
import jax.numpy as jnp
from jax import lax

D = 256
BITS = 18
BLK = 128
OUT_SLOTS = 32
IN_SLOTS = 64
NIN = 16384
N_DP = 64
N_MP = 4


def column_layout(key):
    subkeys = jax.random.split(key, 8)
    capacity = max(1, 2 * OUT_SLOTS // N_DP)
    paired = N_DP // 2
    spread = IN_SLOTS - OUT_SLOTS
    pairing = jax.random.permutation(subkeys[0], N_DP)
    surplus = jax.random.randint(subkeys[1], (paired,), -spread, spread + 1)
    surplus = surplus.at[0].set(spread)
    offsets = jnp.zeros((N_DP,), jnp.int32).at[pairing[:paired]].set(surplus).at[pairing[paired:2 * paired]].set(-surplus)
    live_count = OUT_SLOTS + offsets
    first_serial = jnp.cumsum(live_count) - live_count
    slot_perm = jax.vmap(lambda subkey: jax.random.permutation(subkey, IN_SLOTS))(jax.random.split(subkeys[2], N_DP))
    placed = jnp.argsort(slot_perm, axis=1).astype(jnp.int32)
    is_live = placed < live_count[:, None]
    serial = first_serial[:, None] + placed
    dest_perm = jax.random.permutation(subkeys[3], N_DP).astype(jnp.int32)
    destination = dest_perm[serial // capacity % N_DP]
    arrival = serial // (N_DP * capacity) * capacity + serial % capacity
    land_perm = jax.vmap(lambda subkey: jax.random.permutation(subkey, OUT_SLOTS))(jax.random.split(subkeys[4], N_DP)).astype(jnp.int32)
    landing = land_perm[destination, jnp.clip(arrival, 0, OUT_SLOTS - 1)]
    heights = jax.random.randint(subkeys[5], (N_DP, IN_SLOTS), 8, 65)
    widths = jax.random.randint(subkeys[6], (N_DP, IN_SLOTS), 8, 65)
    partial_value = (heights * widths - 1) % BLK + 1
    complete = jax.random.randint(subkeys[7], (N_DP, IN_SLOTS), 0, 5) < 3
    filled = jnp.where(is_live, jnp.where(complete, BLK, partial_value), 0)
    targets = jnp.where(is_live, destination, -1)
    slots = jnp.where(is_live, landing, -1)
    return jnp.stack([filled, targets, slots]).astype(jnp.int32)


def layout(key):
    columns = jax.vmap(column_layout)(jax.random.split(jax.random.fold_in(key, 11), N_MP))
    return jnp.transpose(columns, (1, 2, 0, 3)).reshape(3, -1)


def draw_fill(key, part):
    return layout(key)[0]


def draw_target(key, part):
    return layout(key)[1]


def draw_target_slot(key, part):
    return layout(key)[2]


def block_scale(key, shape, cuts, least, top_value):
    gain = 1.0
    for dim, shards_of in cuts:
        draws = jax.random.uniform(jax.random.fold_in(jax.random.fold_in(key, 6), dim), (shards_of,), jnp.float32, least / len(cuts), top_value / len(cuts))
        gain = gain * jnp.repeat(jnp.exp(draws), shape[dim] // shards_of).reshape((-1,) + (1,) * (len(shape) - 1 - dim))
    return gain


def gaussian(own_key, dims, deviation, most, shards=(), kind=jnp.bfloat16):
    factor_of = block_scale(own_key, dims, shards, -0.22, 0.18) if shards else 1.0
    entries = jax.random.normal(own_key, dims, jnp.float32) * deviation * factor_of
    return jnp.minimum(jnp.maximum(entries, -most), most).astype(kind)


def setup_inputs(seed: int = 0) -> dict:
    key_list = jax.random.split(jax.random.key(seed), 7)
    latents = gaussian(key_list[0], (NIN * BLK, D), 1.0, 6.0, ((0, 256),))
    proj_weight = gaussian(key_list[1], (BITS, D), D ** -0.5, 0.375)
    proj_bias = gaussian(key_list[2], (BITS,), 0.6, 2.5, (), jnp.float32)
    fill = draw_fill(jax.random.fold_in(key_list[6], 71), 0)
    target = draw_target(jax.random.fold_in(key_list[6], 71), 0)
    target_slot = draw_target_slot(jax.random.fold_in(key_list[6], 71), 0)
    return dict(latents=latents, proj_weight=proj_weight, proj_bias=proj_bias, fill=fill, target=target, target_slot=target_slot)


sharpness = 2.0

def reference(latents, proj_weight, proj_bias, fill, target, target_slot):
    blocks = fill.shape[0]
    token_mask = (jnp.arange(BLK)[None, :] < fill[:, None]).astype(jnp.float32).reshape(-1, 1)
    logits = jnp.dot(latents, proj_weight.T, preferred_element_type=jnp.float32) + proj_bias[None, :]
    scaled = sharpness * logits
    probability = jax.nn.sigmoid(scaled)
    entropy = jax.nn.softplus(scaled) - probability * scaled
    token_count = jnp.sum(fill).astype(jnp.float32)
    marginal = lax.optimization_barrier(jnp.sum(probability * token_mask, axis=0)) / token_count
    entropy_sum = jnp.sum(entropy * token_mask)
    codebook = -jnp.sum(marginal * jnp.log(marginal) + (1.0 - marginal) * jnp.log(1.0 - marginal))
    entropy_loss = entropy_sum / token_count - codebook
    log_odds = jnp.log(1.0 - marginal) - jnp.log(marginal)
    variance = probability * (1.0 - probability) * token_mask
    first_term = -2.0 * scaled * variance
    second_term = 2.0 * variance
    cotangent = (first_term - second_term * log_odds[None, :]).astype(jnp.bfloat16)
    first_rounded = first_term.astype(jnp.bfloat16)
    second_rounded = second_term.astype(jnp.bfloat16)
    contract = (((0,), (0,)), ((), ()))
    first_weight = lax.dot_general(first_rounded, latents, contract, preferred_element_type=jnp.float32)
    second_weight = lax.dot_general(second_rounded, latents, contract, preferred_element_type=jnp.float32)
    weight_grad = (first_weight - second_weight * log_odds[:, None]) / jnp.sqrt(token_count)
    groups = N_DP * N_MP
    grads = lax.map(lambda portion: jnp.dot(portion, proj_weight, preferred_element_type=jnp.float32).astype(jnp.bfloat16), cotangent.reshape(groups, -1, BITS))
    source_block = jnp.arange(blocks).astype(jnp.int32)
    source_mp = source_block // IN_SLOTS % N_MP
    total_out = N_DP * N_MP * OUT_SLOTS
    landing = jnp.where(target >= 0, (target * N_MP + source_mp) * OUT_SLOTS + target_slot, total_out).astype(jnp.int32)
    placed = jnp.zeros((total_out, BLK, D), jnp.bfloat16).at[landing].set(grads.reshape(blocks, BLK, D), mode='drop')
    return (placed.reshape(-1, D), weight_grad, entropy_loss)
```

```python
import jax
import jax.numpy as jnp
from jax import lax
from jax.sharding import Mesh
from jax.sharding import PartitionSpec as P

BLK = 128
OUT_SLOTS = 32
DP = ("dp_0", "dp_1", "dp_2")
DP_MP = ("dp_0", "dp_1", "dp_2", "mp")
LANES = 128

sharpness = 2.0


def routing(fill, target, target_slot, n_dp, n_mp, in_slots, own_dp, own_mp):
    col_shape = (n_dp, n_mp, in_slots)
    col_fill = lax.dynamic_index_in_dim(fill.reshape(col_shape), own_mp, 1, keepdims=False)
    col_target = lax.dynamic_index_in_dim(target.reshape(col_shape), own_mp, 1, keepdims=False)
    col_slot = lax.dynamic_index_in_dim(target_slot.reshape(col_shape), own_mp, 1, keepdims=False)
    own_target = lax.dynamic_index_in_dim(col_target, own_dp, 0, keepdims=False)
    own_fill = lax.dynamic_index_in_dim(col_fill, own_dp, 0, keepdims=False)
    goes = own_target[None, :] == jnp.arange(n_dp, dtype=jnp.int32)[:, None]
    slots = jnp.arange(in_slots, dtype=jnp.int32)[None, :]
    chosen = jnp.sum(jnp.where(goes, slots, 0), axis=1)
    lands = jnp.where(col_target == own_dp, col_slot, -1)
    places = jnp.arange(OUT_SLOTS, dtype=jnp.int32)[:, None, None]
    hits = lands[None] == places
    sources = jnp.arange(n_dp, dtype=jnp.int32)[None, :, None]
    gather_order = jnp.sum(jnp.where(hits, sources, 0), axis=(1, 2))
    out_fill = jnp.sum(jnp.where(hits, col_fill[None], 0), axis=(1, 2))
    return chosen, gather_order, out_fill, own_fill


def token_mask(fills):
    return (lax.broadcasted_iota(jnp.int32, (1, 1, BLK), 2) < fills[:, None, None]).astype(
        jnp.float32
    )


def local(latents, proj_weight, proj_bias, fill, target, target_slot):
    n_dp = lax.axis_size(DP)
    n_mp = lax.axis_size("mp")
    n_all = n_dp * n_mp
    own_dp = lax.axis_index(DP)
    own_mp = lax.axis_index("mp")
    feature_width = latents.shape[1]
    bits = proj_weight.shape[0]
    in_slots = latents.shape[0] // BLK
    chosen, gather_order, out_fill, own_fill = routing(
        fill, target, target_slot, n_dp, n_mp, in_slots, own_dp, own_mp
    )
    token_count = jnp.sum(fill).astype(jnp.float32)
    loaded = latents.reshape(in_slots, BLK, feature_width)
    dots = jnp.einsum("nkd,bd->nbk", loaded, proj_weight, preferred_element_type=jnp.float32)
    outgoing = dots.astype(jnp.float16)[chosen]
    scaled = sharpness * (dots + proj_bias[None, :, None])
    live = token_mask(own_fill)
    probability = jax.nn.sigmoid(scaled)
    entropy = jax.nn.softplus(scaled) - probability * scaled
    bit_sums = jnp.sum(probability * live, axis=(0, 2))
    entropy_sum = jnp.sum(entropy * live)
    variance = probability * (1.0 - probability) * live
    first_rounded = (-2.0 * scaled * variance).astype(jnp.bfloat16)
    second_rounded = (2.0 * variance).astype(jnp.bfloat16)
    first_weight = jnp.einsum(
        "nbk,nkd->db", first_rounded, loaded, preferred_element_type=jnp.float32
    )
    second_weight = jnp.einsum(
        "nbk,nkd->db", second_rounded, loaded, preferred_element_type=jnp.float32
    )
    common = jnp.concatenate([bit_sums, entropy_sum[None]])
    partial = jnp.concatenate(
        [
            first_weight,
            second_weight,
            jnp.broadcast_to(common[None], (feature_width, bits + 1)),
            jnp.zeros((feature_width, LANES - 3 * bits - 1), jnp.float32),
        ],
        axis=1,
    )
    width = feature_width // n_all
    partial = partial.reshape(n_all, width, LANES)
    partials = lax.all_to_all(partial, DP_MP, split_axis=0, concat_axis=0, tiled=True)
    arrived = lax.all_to_all(outgoing, DP, split_axis=0, concat_axis=0, tiled=True)
    sums = jnp.sum(partials, axis=0)
    marginal = sums[0, 2 * bits : 3 * bits] / token_count
    entropy_total = sums[0, 3 * bits]
    codebook = -jnp.sum(marginal * jnp.log(marginal) + (1.0 - marginal) * jnp.log(1.0 - marginal))
    entropy_loss = entropy_total / token_count - codebook
    log_odds = jnp.log(1.0 - marginal) - jnp.log(marginal)
    own_columns = (sums[:, :bits] - sums[:, bits : 2 * bits] * log_odds[None]) / jnp.sqrt(token_count)
    own_columns = jnp.pad(own_columns, ((0, 0), (0, LANES - bits)))
    columns = lax.all_to_all(
        jnp.broadcast_to(own_columns[None], (n_all, width, LANES)),
        DP_MP,
        split_axis=0,
        concat_axis=0,
        tiled=True,
    )
    weight_grad = columns.reshape(feature_width, LANES)[:, :bits].T
    landed = arrived[gather_order].astype(jnp.float32)
    scaled = sharpness * (landed + proj_bias[None, :, None])
    probability = jax.nn.sigmoid(scaled)
    variance = probability * (1.0 - probability) * token_mask(out_fill)
    cotangent = (-2.0 * scaled * variance - 2.0 * variance * log_odds[None, :, None]).astype(
        jnp.bfloat16
    )
    latent_grad = jnp.einsum(
        "nbk,bd->nkd", cotangent, proj_weight, preferred_element_type=jnp.float32
    ).astype(jnp.bfloat16)
    return (latent_grad.reshape(-1, feature_width), weight_grad, entropy_loss)


def solution(mesh):
    torus = Mesh(mesh.devices.reshape(8, 4, 2, mesh.shape["mp"]), DP_MP)
    in_specs = (P(DP_MP, None), P(), P(), P(), P(), P())
    out_specs = (P(DP_MP, None), P(), P())
    return jax.shard_map(local, mesh=torus, in_specs=in_specs, out_specs=out_specs, check_vma=False)
```

```python
import jax
import jax.numpy as jnp
from jax import lax
from jax.sharding import Mesh
from jax.sharding import PartitionSpec as P

BLK = 128
LANES = 128
OUT_SLOTS = 32
DP = ("dp_0", "dp_1", "dp_2")
DP_MP = ("dp_0", "dp_1", "dp_2", "mp")
FINE = 2048.0
ENTROPY_UNIT = 8.0

sharpness = 2.0


def logistic(scaled):
    decay = jnp.exp(-jnp.abs(scaled))
    inverse = 1.0 / (1.0 + decay)
    return decay, inverse, decay * inverse


def token_mask(fills):
    return lax.broadcasted_iota(jnp.int32, (1, 1, BLK), 2) < fills[:, None, None]


def statistics(dots, loaded, proj_bias, own_fill):
    scaled = sharpness * (dots + proj_bias[None, :, None])
    live = token_mask(own_fill)
    decay, inverse, tail = logistic(scaled)
    probability = jnp.where(scaled >= 0.0, inverse, tail)
    entropy = jnp.log1p(decay) + jnp.abs(scaled) * tail
    bit_sums = jnp.sum(jnp.where(live, probability, 0.0), axis=(0, 2))
    entropy_sum = jnp.sum(jnp.where(live, entropy, 0.0))
    second = jnp.where(live, 2.0 * (tail * inverse), 0.0)
    first_weight = jnp.einsum(
        "nbk,nkd->db",
        (-scaled * second).astype(jnp.bfloat16),
        loaded,
        preferred_element_type=jnp.float32,
    )
    second_weight = jnp.einsum(
        "nbk,nkd->db", second.astype(jnp.bfloat16), loaded, preferred_element_type=jnp.float32
    )
    return bit_sums, entropy_sum, first_weight, second_weight


def two_halves(values):
    coarse = values.astype(jnp.float16)
    fine = ((values - coarse.astype(jnp.float32)) * FINE).astype(jnp.float16)
    return coarse, fine


def over_mp(values):
    values = values + lax.ppermute(values, "mp", [(0, 1), (1, 0), (2, 3), (3, 2)])
    return values + lax.ppermute(values, "mp", [(0, 3), (3, 0), (1, 2), (2, 1)])


def landing(fill, target, target_slot, n_dp, in_slots, own_dp, own_mp):
    def column(values):
        return lax.dynamic_slice_in_dim(values.reshape(n_dp, -1), own_mp * in_slots, in_slots, 1)

    col_fill, col_target, col_slot = column(fill), column(target), column(target_slot)
    lands = jnp.where(col_target == own_dp, col_slot, -1)
    places = jnp.arange(OUT_SLOTS, dtype=jnp.int32)[:, None, None]
    hits = lands[None] == places
    sources = jnp.arange(n_dp, dtype=jnp.int32)[None, :, None]
    gather_order = jnp.sum(jnp.where(hits, sources, 0), axis=(1, 2))
    out_fill = jnp.sum(jnp.where(hits, col_fill[None], 0), axis=(1, 2))
    return gather_order, out_fill


def local(latents, proj_weight, proj_bias, fill, target, target_slot):
    n_dp = lax.axis_size(DP)
    n_mp = lax.axis_size("mp")
    own_dp = lax.axis_index(DP)
    own_mp = lax.axis_index("mp")
    width = latents.shape[1]
    bits = proj_weight.shape[0]
    in_slots = latents.shape[0] // BLK
    parts = width // n_dp
    own_start = (own_dp * n_mp + own_mp) * in_slots
    own_target = lax.dynamic_slice_in_dim(target, own_start, in_slots)
    own_fill = lax.dynamic_slice_in_dim(fill, own_start, in_slots)
    goes = own_target[None, :] == jnp.arange(n_dp, dtype=jnp.int32)[:, None]
    chosen = jnp.sum(jnp.where(goes, jnp.arange(in_slots, dtype=jnp.int32)[None, :], 0), axis=1)
    loaded = latents.reshape(in_slots, BLK, width)
    dots = jnp.einsum("nkd,bd->nbk", loaded, proj_weight, preferred_element_type=jnp.float32)
    bit_sums, entropy_sum, first_weight, second_weight = statistics(
        dots, loaded, proj_bias, own_fill
    )
    common = jnp.concatenate([bit_sums, entropy_sum[None] / ENTROPY_UNIT])
    common = jnp.broadcast_to(common[None], (width, bits + 1))
    partial = jnp.concatenate([first_weight, second_weight, common], axis=1)
    coarse, fine = two_halves(partial)
    used = 3 * bits + 1
    coarse = jnp.pad(coarse, ((0, 0), (0, LANES // 2 - used)))
    fine = jnp.pad(fine, ((0, 0), (0, LANES // 2 - used)))
    partial = jnp.concatenate([coarse, fine], axis=1)
    partial = jnp.transpose(partial.reshape(parts, n_dp, LANES), (1, 0, 2))
    outgoing = jnp.concatenate([dots.astype(jnp.float16)[chosen], partial], axis=1)
    arrived = lax.all_to_all(outgoing, DP, split_axis=0, concat_axis=0, tiled=True)
    token_count = jnp.sum(fill).astype(jnp.float32)
    gather_order, out_fill = landing(fill, target, target_slot, n_dp, in_slots, own_dp, own_mp)
    sums = jnp.sum(arrived[:, bits:].astype(jnp.float32), axis=0)
    sums = sums[:, : LANES // 2] + sums[:, LANES // 2 :] / FINE
    sums = over_mp(sums)
    totals = sums[0]
    marginal = totals[2 * bits : 3 * bits] / token_count
    log_odds = jnp.log(1.0 - marginal) - jnp.log(marginal)
    codebook = -jnp.sum(marginal * jnp.log(marginal) + (1.0 - marginal) * jnp.log(1.0 - marginal))
    entropy_loss = totals[3 * bits] * ENTROPY_UNIT / token_count - codebook
    columns = sums[:, :bits] - sums[:, bits : 2 * bits] * log_odds[None]
    columns = (columns / jnp.sqrt(token_count)).reshape(1, parts * bits)
    columns = jnp.pad(columns, ((0, 0), (0, LANES - parts * bits)))
    columns = lax.all_to_all(
        jnp.broadcast_to(columns[None], (n_dp, 1, LANES)), DP, split_axis=0, concat_axis=0, tiled=True
    )
    columns = columns.reshape(n_dp, LANES)[:, : parts * bits].T.reshape(parts, bits, n_dp)
    weight_grad = jnp.transpose(columns, (1, 0, 2)).reshape(bits, width)
    landed = arrived[gather_order][:, :bits].astype(jnp.float32)
    scaled = sharpness * (landed + proj_bias[None, :, None])
    _, inverse, tail = logistic(scaled)
    second = jnp.where(token_mask(out_fill), 2.0 * (tail * inverse), 0.0)
    cotangent = (-second * (scaled + log_odds[None, :, None])).astype(jnp.bfloat16)
    latent_grad = jnp.einsum(
        "nbk,bd->nkd", cotangent, proj_weight, preferred_element_type=jnp.float32
    ).astype(jnp.bfloat16)
    return (latent_grad.reshape(-1, width), weight_grad, entropy_loss)


def solution(mesh):
    torus = Mesh(mesh.devices.reshape(8, 4, 2, mesh.shape["mp"]), DP_MP)
    in_specs = (P(DP_MP, None), P(), P(), P(), P(), P())
    out_specs = (P(DP_MP, None), P(), P())
    return jax.shard_map(local, mesh=torus, in_specs=in_specs, out_specs=out_specs, check_vma=False)
```

```python
import jax
import jax.numpy as jnp
from jax import lax
from jax.experimental import pallas as pl
from jax.experimental.pallas import tpu as pltpu
from jax.sharding import Mesh
from jax.sharding import PartitionSpec as P


BLK = 128
LANES = 128
OUT_SLOTS = 32
DP = ("dp_0", "dp_1", "dp_2")
DP_MP = ("dp_0", "dp_1", "dp_2", "mp")
FINE = 256.0
ENTROPY_UNIT = 8.0
CHUNK_SLOTS = 8
WINDOW = 1024
SECOND_LANE = 24
COMMON_LANE = 42

sharpness = 2.0


def logistic(scaled):
    decay = jnp.exp(-jnp.abs(scaled))
    inverse = 1.0 / (1.0 + decay)
    return decay, inverse, decay * inverse


def token_mask(fills):
    return lax.broadcasted_iota(jnp.int32, (1, 1, BLK), 2) < fills[:, None, None]


def diagonal(shape, offset=0):
    rows = lax.broadcasted_iota(jnp.int32, shape, 0)
    return rows + offset == lax.broadcasted_iota(jnp.int32, shape, 1)


def front_kernel(
    fill_hbm, target_hbm, bias_ref, latents_hbm, weight_ref, sent_ref, sums_ref,
    fill_ref, target_ref, lhs, latents, arrivals, tables,
):
    in_slots = latents_hbm.shape[0] // BLK
    bits = weight_ref.shape[0]
    tokens = CHUNK_SLOTS * BLK
    chunks = in_slots // CHUNK_SLOTS

    def fetch(chunk):
        rows = pl.ds(chunk * tokens, tokens)
        return pltpu.make_async_copy(latents_hbm.at[rows], latents.at[rows], arrivals.at[chunk])

    own_start = lax.axis_index(DP_MP) * in_slots
    window = fill_ref.shape[0]
    own_window = pl.ds(pl.multiple_of(own_start // window * window, window), window)
    own_offset = own_start % window
    fill_copy = pltpu.make_async_copy(fill_hbm.at[own_window], fill_ref, tables.at[0])
    target_copy = pltpu.make_async_copy(target_hbm.at[own_window], target_ref, tables.at[1])
    fill_copy.start()
    target_copy.start()
    for chunk in range(chunks):
        fetch(chunk).start()
    lhs[...] = jnp.zeros_like(lhs)
    rows = lax.broadcasted_iota(jnp.int32, (bits, BLK), 0)
    bias = jnp.zeros((bits, BLK), jnp.float32)
    for bit in range(bits):
        bias = jnp.where(rows == bit, bias_ref[bit], bias)
    spare = sent_ref.shape[0] - 1
    fill_copy.wait()
    target_copy.wait()
    lanes = lax.broadcasted_iota(jnp.int32, (1, BLK), 1)
    bit_acc = jnp.zeros((bits, BLK), jnp.float32)
    ent_acc = jnp.zeros((bits, BLK), jnp.float32)
    acc = jnp.zeros((lhs.shape[1], weight_ref.shape[1]), jnp.float32)

    def project(chunk):
        fetch(chunk).wait()
        return lax.dot_general(
            weight_ref[...],
            latents[chunk * tokens : (chunk + 1) * tokens],
            (((1,), (1,)), ((), ())),
            preferred_element_type=jnp.float32,
        )

    ahead = project(0)
    for chunk in range(chunks):
        dots = ahead
        if chunk + 1 < chunks:
            ahead = project(chunk + 1)
        for i in range(CHUNK_SLOTS):
            slot = chunk * CHUNK_SLOTS + i
            span = slice(i * BLK, (i + 1) * BLK)
            piece = dots[:, span]
            place = target_ref[own_offset + slot]
            sent_ref[jnp.where(place >= 0, place, spare)] = piece
            scaled = sharpness * (piece + bias)
            live = lanes < fill_ref[own_offset + slot]
            decay, inverse, tail = logistic(scaled)
            probability = jnp.where(scaled >= 0.0, inverse, tail)
            raised = 1.0 + decay
            log1p = jnp.log(raised) + (decay - (raised - 1.0)) * inverse
            entropy = log1p + jnp.abs(scaled) * tail
            second = jnp.where(live, 2.0 * (tail * inverse), 0.0)
            bit_acc += jnp.where(live, probability, 0.0)
            ent_acc += jnp.where(live, entropy, 0.0)
            lhs[chunk % 2, :bits, span] = (-scaled * second).astype(lhs.dtype)
            lhs[chunk % 2, SECOND_LANE : SECOND_LANE + bits, span] = second.astype(lhs.dtype)
        acc += lax.dot_general(
            lhs[chunk % 2],
            latents[chunk * tokens : (chunk + 1) * tokens],
            (((1,), (0,)), ((), ())),
            preferred_element_type=jnp.float32,
        )
    width = acc.shape[1]
    bit_sums = jnp.sum(bit_acc, axis=1, keepdims=True)
    entropy_sum = jnp.sum(jnp.sum(ent_acc, axis=1, keepdims=True), axis=0, keepdims=True)
    common = jnp.sum(
        jnp.where(diagonal((bits, LANES), COMMON_LANE), bit_sums, 0.0), axis=0, keepdims=True
    )
    common = jnp.where(lanes == COMMON_LANE + bits, entropy_sum / ENTROPY_UNIT, common)
    spread = jnp.concatenate([acc, jnp.zeros((LANES - acc.shape[0], width), jnp.float32)], axis=0)
    partial = jnp.where(lanes < COMMON_LANE, jnp.transpose(spread), common)
    coarse = partial.astype(jnp.bfloat16).astype(jnp.float32)
    fine = (partial - coarse) * FINE
    half = LANES // 2
    sums_ref[...] = jnp.where(lanes < half, coarse, pltpu.roll(fine, half, 1))


def front(latents, proj_weight, proj_bias, fill, target, n_dp):
    rows, width = latents.shape
    bits = proj_weight.shape[0]
    in_slots = rows // BLK
    hbm = pl.BlockSpec(memory_space=pl.ANY)
    smem = pl.BlockSpec(memory_space=pltpu.SMEM)
    vmem = pl.BlockSpec(memory_space=pltpu.VMEM)
    return pl.pallas_call(
        front_kernel,
        in_specs=[hbm, hbm, smem, hbm, vmem],
        out_specs=[vmem, vmem],
        out_shape=[
            pltpu.VMEM((n_dp + 1, bits, BLK), jnp.float32),
            pltpu.VMEM((width, LANES), jnp.float32),
        ],
        scratch_shapes=[
            pltpu.SMEM((WINDOW,), jnp.int32),
            pltpu.SMEM((WINDOW,), jnp.int32),
            pltpu.VMEM((2, LANES // 2, CHUNK_SLOTS * BLK), jnp.bfloat16),
            pltpu.VMEM((rows, width), jnp.bfloat16),
            pltpu.SemaphoreType.DMA((in_slots // CHUNK_SLOTS,)),
            pltpu.SemaphoreType.DMA((2,)),
        ],
        name="front",
    )(fill, target, proj_bias, latents, proj_weight)


def over_mp(values):
    values = values + lax.ppermute(values, "mp", [(0, 1), (1, 0), (2, 3), (3, 2)])
    return values + lax.ppermute(values, "mp", [(0, 3), (3, 0), (1, 2), (2, 1)])


def landing(fill, target, target_slot, n_dp, in_slots, own_dp, own_mp):
    def column(values):
        return lax.dynamic_slice_in_dim(values.reshape(n_dp, -1), own_mp * in_slots, in_slots, 1)

    col_fill, col_target, col_slot = column(fill), column(target), column(target_slot)
    lands = jnp.where(col_target == own_dp, col_slot, -1)
    places = jnp.arange(OUT_SLOTS, dtype=jnp.int32)[:, None, None]
    hits = lands[None] == places
    sources = jnp.arange(n_dp, dtype=jnp.int32)[None, :, None]
    gather_order = jnp.sum(jnp.where(hits, sources, 0), axis=(1, 2))
    out_fill = jnp.sum(jnp.where(hits, col_fill[None], 0), axis=(1, 2))
    return gather_order, out_fill


def local(latents, proj_weight, proj_bias, fill, target, target_slot):
    n_dp = lax.axis_size(DP)
    own_dp = lax.axis_index(DP)
    own_mp = lax.axis_index("mp")
    width = latents.shape[1]
    bits = proj_weight.shape[0]
    in_slots = latents.shape[0] // BLK
    parts = width // n_dp
    sent, partial = front(latents, proj_weight, proj_bias, fill, target, n_dp)
    partial = jnp.transpose(partial.reshape(parts, n_dp, LANES), (1, 0, 2))
    outgoing = jnp.concatenate([sent[:n_dp], partial], axis=1).astype(jnp.float16)
    outgoing = outgoing.reshape(n_dp, 2, -1)
    arrived = lax.all_to_all(outgoing, DP, split_axis=0, concat_axis=0, tiled=True)
    arrived = arrived.reshape(n_dp, -1, BLK)
    token_count = jnp.sum(fill).astype(jnp.float32)
    gather_order, out_fill = landing(fill, target, target_slot, n_dp, in_slots, own_dp, own_mp)
    arrived, token_count, root_count, gather_order, out_fill = lax.optimization_barrier(
        (arrived, token_count, jnp.sqrt(token_count), gather_order, out_fill)
    )
    sums = jnp.sum(arrived[:, bits:].astype(jnp.float32), axis=0)
    sums = sums[:, : LANES // 2] + sums[:, LANES // 2 :] / FINE
    sums = over_mp(sums)
    marginal = sums[0, COMMON_LANE : COMMON_LANE + bits] / token_count
    log_odds = jnp.log(1.0 - marginal) - jnp.log(marginal)
    columns = sums[:, :bits] - sums[:, SECOND_LANE : SECOND_LANE + bits] * log_odds[None]
    columns = (columns / root_count).reshape(1, parts * bits)
    columns = jnp.pad(columns, ((0, 0), (0, LANES - parts * bits)))
    columns = jnp.broadcast_to(columns[None], (n_dp, 1, LANES))
    columns = lax.all_to_all(columns, DP, split_axis=0, concat_axis=0, tiled=True)
    columns = columns.reshape(n_dp, LANES)[:, : parts * bits].T.reshape(parts, bits, n_dp)
    weight_grad = jnp.transpose(columns, (1, 0, 2)).reshape(bits, width)
    landed = arrived[gather_order][:, :bits].astype(jnp.float32)
    scaled = sharpness * (landed + proj_bias[None, :, None])
    _, inverse, tail = logistic(scaled)
    second = jnp.where(token_mask(out_fill), 2.0 * (tail * inverse), 0.0)
    cotangent = (-second * (scaled + log_odds[None, :, None])).astype(jnp.bfloat16)
    latent_grad = jnp.einsum(
        "nbk,bd->nkd", cotangent, proj_weight, preferred_element_type=jnp.float32
    ).astype(jnp.bfloat16)
    sums, latent_grad = lax.optimization_barrier((sums, latent_grad))
    totals = sums[0, COMMON_LANE : COMMON_LANE + bits + 1] / token_count
    is_bit = jnp.arange(bits + 1) < bits
    marginal = jnp.where(is_bit, totals, 0.5)
    negative = marginal * jnp.log(marginal) + (1.0 - marginal) * jnp.log(1.0 - marginal)
    entropy_loss = jnp.sum(jnp.where(is_bit, negative, totals * ENTROPY_UNIT))
    return (latent_grad.reshape(-1, width), weight_grad, entropy_loss)


def solution(mesh):
    torus = Mesh(mesh.devices.reshape(8, 4, 2, mesh.shape["mp"]), DP_MP)
    in_specs = (P(DP_MP, None), P(), P(), P(), P(), P())
    out_specs = (P(DP_MP, None), P(), P())
    return jax.shard_map(local, mesh=torus, in_specs=in_specs, out_specs=out_specs, check_vma=False)
```
